32 devices in a mesh: grp: 2 (over y), pulse: 4 (over z), chan: 2 (over x), sub: 2 (over core).
Axes of the slice: x: 2, y: 2, z: 4, core: 2. Of those that a mesh axis runs over, the one named last changes fastest.
Arguments:
- samples: int32 [2, 16, 512, 4096], P(None, ('grp', 'chan', 'sub'), 'pulse'), parts along dimension 1, may hold values from -2048 to 2047
- replica: float32 [2, 4096], replicated, may hold values from -6 to 6
- window: int32 [16, 2], P(('grp', 'chan', 'sub')), parts along dimension 0, may hold values from 1 to 28, as said below
- thresh: int32 [16, 2], P(('grp', 'chan', 'sub')), parts along dimension 0, may hold values from 2 to 32, as said below
Outputs:
- ratio_map: float32 [16, 512, 4096], P(('grp', 'chan', 'sub'), None, 'pulse'), parts along dimension 0
- detections: float32 [2], P('grp'), parts along dimension 0
The draws below stay inside these ranges and needn't reach their ends.
There are 2 independent parts, one for each index of `grp`. The reference program is written for one: setup_inputs(seed, part) draws one part's arguments, and reference() takes and returns one part's arrays. A program takes and returns all parts, laid end to end along the dimension named above; an argument that names none is the same for every part. Nothing has to cross between parts.
Inputs may be any that keep to these rules, and one draw needn't show every extreme that they name: `window`: column 0 is a channel's guard gates on each side, 1 to 4; column 1 its training gates on each side, 14 to 28; some channel has both at their most. `thresh`: column 0 is a numerator of 8 to 32, column 1 a denominator of 2 to 4.
All inputs are finite; a program needn't handle non-finite values.
Results may differ from the reference program's by a relative error of at most 0.0003.
Values sent between devices are 32-bit elements; how exact they have to be, the bound alone decides.
A program may use at most 128 MiB of HBM per device.

```python
import jax
import jax.numpy as jnp
from jax import lax

PULSES = 512
RANGE = 4096
GUARD_MAX = 4
TRAIN_MAX = 28
CHANNELS = 8


def draw_window(key, part):
    guard_key, train_key, pick_key = jax.random.split(jax.random.fold_in(key, 11), 3)
    guards = jax.random.randint(guard_key, (CHANNELS,), 1, GUARD_MAX + 1)
    trains = jax.random.randint(train_key, (CHANNELS,), TRAIN_MAX // 2, TRAIN_MAX + 1)
    chosen = jax.random.randint(pick_key, (), 0, CHANNELS)
    is_pick = jnp.arange(CHANNELS) == chosen
    guards = jnp.where(is_pick, GUARD_MAX, guards)
    trains = jnp.where(is_pick, TRAIN_MAX, trains)
    return jnp.stack([guards, trains], axis=1).astype(jnp.int32)


def draw_thresh(key, part):
    num_key, den_key = jax.random.split(jax.random.fold_in(key, 23))
    numerators = jax.random.randint(num_key, (CHANNELS,), 8, 33)
    denominators = jax.random.randint(den_key, (CHANNELS,), 2, 5)
    return jnp.stack([numerators, denominators], axis=1).astype(jnp.int32)


def with_ends(array, rng, least, top_value):
    longest = array.shape.index(max(array.shape))
    spots = []
    for shift in (0, 1):
        where = [jax.random.randint(jax.random.fold_in(rng, axis), (), 0, length) for axis, length in enumerate(array.shape)]
        where[longest] = (where[longest] + shift) % array.shape[longest]
        spots.append(tuple(where))
    return array.at[spots[0]].set(least).at[spots[1]].set(top_value)


def gaussian(key, shape, spread, bound, kind=jnp.bfloat16):
    array = jax.random.normal(key, shape, jnp.float32) * spread
    return jnp.minimum(jnp.maximum(array, -bound), bound).astype(kind)


def setup_inputs(seed: int = 0, part: int = 0) -> dict:
    key_of = jax.random.split(jax.random.key(seed), 5)
    own_keys = jax.random.split(jax.random.fold_in(key_of[4], part), 5)
    samples = with_ends(jax.random.randint(own_keys[0], (2, CHANNELS, PULSES, RANGE), -2048, 2048), jax.random.fold_in(own_keys[0], 1), -2048, 2047).astype(jnp.int32)
    replica = gaussian(key_of[1], (2, RANGE), 1.0, 6.0, jnp.float32)
    window = draw_window(jax.random.fold_in(jax.random.fold_in(key_of[4], part), 71), part)
    thresh = draw_thresh(jax.random.fold_in(jax.random.fold_in(key_of[4], part), 71), part)
    return {"samples": samples, "replica": replica, "window": window, "thresh": thresh}


def reference(samples, replica, window, thresh):
    margin = GUARD_MAX + TRAIN_MAX
    filt = lax.complex(replica[0], replica[1])

    def per_channel(index):
        chan_samples = lax.dynamic_index_in_dim(samples, index, 1, keepdims=False)
        chan_window = lax.dynamic_index_in_dim(window, index, 0, keepdims=False)
        chan_thresh = lax.dynamic_index_in_dim(thresh, index, 0, keepdims=False)
        signal = lax.complex(chan_samples[0].astype(jnp.float32) / 2048.0, chan_samples[1].astype(jnp.float32) / 2048.0)
        spectrum = jnp.fft.fft(signal, axis=-1, norm="ortho")
        compressed = jnp.fft.ifft(spectrum * filt[None, :], axis=-1, norm="ortho")
        doppler = jnp.fft.fft(compressed, axis=0, norm="ortho")
        power = jnp.real(doppler) ** 2 + jnp.imag(doppler) ** 2
        guard = chan_window[0]
        train = chan_window[1]
        padded = jnp.pad(power, ((0, 0), (margin, margin)))
        inside = jnp.pad(jnp.ones((RANGE,), jnp.float32), (margin, margin))
        noise_sum = jnp.zeros_like(power)
        cells = jnp.zeros((RANGE,), jnp.float32)
        for offset in range(1, margin + 1):
            weight = ((offset > guard) & (offset <= guard + train)).astype(jnp.float32)
            noise_sum = noise_sum + weight * (padded[:, margin + offset:margin + offset + RANGE] + padded[:, margin - offset:margin - offset + RANGE])
            cells = cells + weight * (inside[margin + offset:margin + offset + RANGE] + inside[margin - offset:margin - offset + RANGE])
        level = (noise_sum + 1e-6) / cells[None, :]
        ratio = power / level
        scale = chan_thresh[0].astype(jnp.float32) / chan_thresh[1].astype(jnp.float32)
        soft = jnp.clip(ratio / scale - 1.0, 0.0, 1.0)
        return ratio, jnp.sum(soft)

    ratio_map, soft_sums = lax.map(per_channel, jnp.arange(CHANNELS, dtype=jnp.int32))
    detections = jnp.sum(soft_sums) * (1024.0 / (PULSES * RANGE))
    return ratio_map, detections.reshape(1)
```

```python
import functools
import math

import jax
import jax.numpy as jnp
import numpy as np
from jax import lax
from jax.experimental import pallas as pl
from jax.experimental.pallas import tpu as pltpu
from jax.sharding import PartitionSpec as P

GUARD_MAX = 4
TRAIN_MAX = 28
MARGIN = GUARD_MAX + TRAIN_MAX
EPSILON = 1e-06
INPUT_SCALE = 1.0 / 2048.0
LANES = 128
SUB = 8
RADIX = 4


def halves(table):
    hi = np.asarray(table, np.float32).astype(jnp.bfloat16)
    lo = (np.asarray(table, np.float64) - hi.astype(np.float64)).astype(jnp.bfloat16)
    return hi, lo


def lane_table(sign):
    idx = np.arange(LANES)
    ang = 2.0 * np.pi * ((idx[:, None] * idx[None, :]) % LANES) / LANES
    c, s = np.cos(ang), sign * np.sin(ang)
    full = np.block([[c, s], [-s, c]])
    hi, lo = halves(full)
    return np.concatenate([hi, hi, lo], axis=0)


def doppler_table(pulses):
    part = pulses // RADIX
    m = np.arange(part)
    out = []
    for res in range(RADIX):
        ang = 2.0 * np.pi * ((m[None, :] * (RADIX * m[:, None] + res)) % pulses) / pulses
        c, s = np.cos(ang) / math.sqrt(pulses), -np.sin(ang) / math.sqrt(pulses)
        full = np.block([[c, -s], [s, c]])
        hi, lo = halves(full)
        out.append(np.concatenate([hi, hi, lo], axis=1))
    return np.stack(out)


def split(x, axis):
    hi = x.astype(jnp.bfloat16)
    lo = (x - hi.astype(jnp.float32)).astype(jnp.bfloat16)
    return jnp.concatenate([hi, lo, hi], axis=axis)


def fft_list(re, im, sign):
    n = len(re)
    if n == 1:
        return re, im
    er, ei = fft_list(re[0::2], im[0::2], sign)
    odd_r, odd_i = fft_list(re[1::2], im[1::2], sign)
    half = n // 2
    out_r, out_i = [None] * n, [None] * n
    for k in range(half):
        a, b = odd_r[k], odd_i[k]
        if k == 0:
            tr, ti = a, b
        elif 4 * k == n:
            tr, ti = (b, -a) if sign < 0 else (-b, a)
        elif 8 * k == n or 8 * k == 3 * n:
            h = math.sqrt(0.5)
            c = h if 8 * k == n else -h
            tr = c * a - (sign * h) * b
            ti = c * b + (sign * h) * a
        else:
            c = math.cos(2.0 * math.pi * k / n)
            s = sign * math.sin(2.0 * math.pi * k / n)
            tr = c * a - s * b
            ti = s * a + c * b
        out_r[k], out_i[k] = er[k] + tr, ei[k] + ti
        out_r[k + half], out_i[k + half] = er[k] - tr, ei[k] - ti
    return out_r, out_i


def range_kernel(n, rows, x_ref, tw1, rep, tw2, wf, wi, *rest):
    outs = rest[:n]
    cols = x_ref.shape[-1] // LANES
    per = cols // n

    def body(g, carry):
        r0 = pl.multiple_of(g * SUB, SUB)
        re = [x_ref[0, 0, pl.ds(r0, SUB), a * LANES:(a + 1) * LANES].astype(jnp.float32) for a in range(cols)]
        im = [x_ref[1, 0, pl.ds(r0, SUB), a * LANES:(a + 1) * LANES].astype(jnp.float32) for a in range(cols)]
        re, im = fft_list(re, im, -1.0)
        mr, mi = jnp.concatenate(re, axis=0), jnp.concatenate(im, axis=0)
        tr, ti = tw1[0], tw1[1]
        m = jnp.concatenate([mr * tr - mi * ti, mr * ti + mi * tr], axis=1)
        f = jnp.dot(split(m, 1), wf[...], preferred_element_type=jnp.float32)
        fr, fi = f[:, :LANES], f[:, LANES:]
        tr, ti = rep[0], rep[1]
        m = jnp.concatenate([fr * tr - fi * ti, fr * ti + fi * tr], axis=1)
        f = jnp.dot(split(m, 1), wi[...], preferred_element_type=jnp.float32)
        fr, fi = f[:, :LANES], f[:, LANES:]
        tr, ti = tw2[0], tw2[1]
        mr, mi = fr * tr - fi * ti, fr * ti + fi * tr
        re = [mr[a * SUB:(a + 1) * SUB] for a in range(cols)]
        im = [mi[a * SUB:(a + 1) * SUB] for a in range(cols)]
        re, im = fft_list(re, im, 1.0)
        for j in range(n):
            for a in range(per):
                outs[j][0, pl.ds(r0, SUB), a * LANES:(a + 1) * LANES] = re[j * per + a]
                outs[j][1, pl.ds(r0, SUB), a * LANES:(a + 1) * LANES] = im[j * per + a]
        return carry

    lax.fori_loop(0, rows // SUB, body, 0, unroll=2)


def range_compress(n, channel, samples, tw1, rep, tw2, wf, wi):
    _, _, pulses, gates = samples.shape
    rows = min(32, pulses)
    whole = lambda a: pl.BlockSpec(a.shape, lambda i: (0,) * a.ndim)
    return pl.pallas_call(
        functools.partial(range_kernel, n, rows),
        grid=(pulses // rows,),
        in_specs=[pl.BlockSpec((2, 1, rows, gates), lambda i: (0, channel, i, 0))]
        + [whole(a) for a in (tw1, rep, tw2, wf, wi)],
        out_specs=[pl.BlockSpec((2, rows, gates // n), lambda i: (0, i, 0))] * n,
        out_shape=[jax.ShapeDtypeStruct((2, pulses, gates // n), jnp.float32)] * n,
        compiler_params=pltpu.CompilerParams(vmem_limit_bytes=40 << 20),
        cost_estimate=pl.CostEstimate(flops=int(3e9), bytes_accessed=16 << 20, transcendentals=0),
    )(samples, tw1, rep, tw2, wf, wi)


def doppler_kernel(x0, x1, x2, x3, t_ref, p_ref):
    part = x0.shape[1]
    a, b, c, d = ([x[0], x[1]] for x in (x0, x1, x2, x3))
    sr, si = a[0] + c[0], a[1] + c[1]
    dr, di = a[0] - c[0], a[1] - c[1]
    ur, ui = b[0] + d[0], b[1] + d[1]
    vr, vi = b[0] - d[0], b[1] - d[1]
    ys = [(sr + ur, si + ui), (dr + vi, di - vr), (sr - ur, si - ui), (dr - vi, di + vr)]
    for res in range(RADIX):
        y = jnp.concatenate(ys[res], axis=0)
        out = jnp.dot(t_ref[res], split(y, 0), preferred_element_type=jnp.float32)
        re, im = out[:part], out[part:]
        p_ref[res] = re * re + im * im


def doppler_power(blocks, table):
    _, part, gates = blocks[0].shape
    width = min(256, gates)
    return pl.pallas_call(
        doppler_kernel,
        grid=(gates // width,),
        in_specs=[pl.BlockSpec((2, part, width), lambda i: (0, 0, i))] * RADIX
        + [pl.BlockSpec(table.shape, lambda i: (0, 0, 0))],
        out_specs=pl.BlockSpec((RADIX, part, width), lambda i: (0, 0, i)),
        out_shape=jax.ShapeDtypeStruct((RADIX, part, gates), jnp.float32),
        compiler_params=pltpu.CompilerParams(vmem_limit_bytes=40 << 20),
        cost_estimate=pl.CostEstimate(flops=int(3e9), bytes_accessed=8 << 20, transcendentals=0),
    )(*blocks, table)


def cfar_kernel(channel, scale_ref, p_ref, l_ref, r_ref, band_ref, cells_ref, *rest):
    out_ref, sum_ref, turn = rest[-3:]
    _, rows, gates = p_ref.shape
    width = band_ref.shape[-1]
    total = RADIX * rows
    core = p_ref[...].reshape(total, gates)
    zeros = jnp.zeros((total, LANES - MARGIN), jnp.float32)
    padded = jnp.concatenate(
        [zeros, l_ref[...].reshape(total, MARGIN), core, r_ref[...].reshape(total, MARGIN), zeros], axis=1
    )
    hi = padded.astype(jnp.bfloat16)
    lo = (padded - hi.astype(jnp.float32)).astype(jnp.bfloat16)
    band = band_ref[0]
    inv = scale_ref[channel, 1].astype(jnp.float32) / scale_ref[channel, 0].astype(jnp.float32)
    acc = jnp.zeros((SUB, LANES), jnp.float32)
    for g in range(gates // width):
        cut = slice(g * width, (g + 1) * width + 2 * LANES)
        noise = jnp.dot(hi[:, cut], band, preferred_element_type=jnp.float32) + jnp.dot(
            lo[:, cut], band, preferred_element_type=jnp.float32
        )
        here = slice(g * width, (g + 1) * width)
        ratio = core[:, here] * cells_ref[0, :, here] / (noise + EPSILON)
        for c in range(width // LANES):
            lanes = slice(c * LANES, (c + 1) * LANES)
            for res in range(RADIX):
                turn[g, c, pl.ds(res, rows, stride=RADIX), :] = ratio[res * rows:(res + 1) * rows, lanes]
            out_ref[0, :, g * width + c * LANES:g * width + (c + 1) * LANES] = turn[g, c]
        soft = jnp.clip(ratio * inv - 1.0, 0.0, 1.0)
        for c in range(width // LANES):
            acc = acc + jnp.sum(soft[:, c * LANES:(c + 1) * LANES].reshape(total // SUB, SUB, LANES), axis=0)

    @pl.when(pl.program_id(0) == 0)
    def _():
        sum_ref[...] = jnp.zeros_like(sum_ref)

    sum_ref[...] += acc


def cfar(channel, channels, power, left, right, band, cells, thresh, prior):
    _, part, gates = power.shape
    rows = min(32, part)
    width = band.shape[-1]
    specs = [
        pl.BlockSpec(memory_space=pltpu.SMEM),
        pl.BlockSpec((RADIX, rows, gates), lambda i: (0, i, 0)),
        pl.BlockSpec((RADIX, rows, MARGIN), lambda i: (0, i, 0)),
        pl.BlockSpec((RADIX, rows, MARGIN), lambda i: (0, i, 0)),
        pl.BlockSpec((1,) + band.shape[1:], lambda i: (channel, 0, 0)),
        pl.BlockSpec((1,) + cells.shape[1:], lambda i: (channel, 0, 0)),
    ]
    args = [thresh, power, left, right, band, cells]
    aliases = {}
    if prior is not None:
        specs.append(pl.BlockSpec(memory_space=pl.ANY))
        args.append(prior)
        aliases = {6: 0}
    return pl.pallas_call(
        functools.partial(cfar_kernel, channel),
        grid=(part // rows,),
        in_specs=specs,
        out_specs=[
            pl.BlockSpec((1, RADIX * rows, gates), lambda i: (channel, i, 0)),
            pl.BlockSpec((SUB, LANES), lambda i: (0, 0)),
        ],
        out_shape=[
            jax.ShapeDtypeStruct((channels, RADIX * part, gates), jnp.float32),
            jax.ShapeDtypeStruct((SUB, LANES), jnp.float32),
        ],
        input_output_aliases=aliases,
        scratch_shapes=[pltpu.VMEM((gates // width, width // LANES, RADIX * rows, LANES), jnp.float32)],
        compiler_params=pltpu.CompilerParams(vmem_limit_bytes=40 << 20),
        cost_estimate=pl.CostEstimate(flops=int(2e9), bytes_accessed=5 << 20, transcendentals=0),
    )(*args)


def local(samples, replica, window, thresh):
    _, channels, part, gates = samples.shape
    n = lax.axis_size("pulse")
    me = lax.axis_index("pulse")
    cols = gates // LANES
    pulses = part * n
    own = gates // n

    k1 = np.arange(cols)[:, None]
    b = np.arange(LANES)[None, :]
    ang = 2.0 * np.pi * ((k1 * b) % gates) / gates
    tw1 = np.repeat(np.stack([np.cos(ang), -np.sin(ang)]), SUB, axis=1).astype(np.float32)
    turned = (jnp.asarray(k1 * b, jnp.int32) + own * me * jnp.asarray(k1, jnp.int32)) % gates
    ang2 = turned.astype(jnp.float32) * (2.0 * math.pi / gates)
    tw2 = jnp.repeat(jnp.stack([jnp.cos(ang2), jnp.sin(ang2)]), SUB, axis=1)
    rep = jnp.swapaxes(replica.reshape(2, LANES, cols), 1, 2) * (INPUT_SCALE / gates)
    rep = jnp.repeat(rep, SUB, axis=1)
    wf, wi = jnp.asarray(lane_table(-1.0)), jnp.asarray(lane_table(1.0))
    table = jnp.asarray(doppler_table(pulses))

    width = min(256, own)
    guard = window[:, 0][:, None, None]
    reach = guard + window[:, 1][:, None, None]
    dist = jnp.abs(
        jnp.arange(width + 2 * LANES, dtype=jnp.int32)[:, None] - LANES - jnp.arange(width, dtype=jnp.int32)[None, :]
    )[None]
    band = ((dist > guard) & (dist <= reach)).astype(jnp.bfloat16)
    gate = (me * own + jnp.arange(own, dtype=jnp.int32))[None, None, :]
    after = gates - 1 - gate
    cells = (
        jnp.minimum(gate, reach) - jnp.minimum(gate, guard) + jnp.minimum(after, reach) - jnp.minimum(after, guard)
    ).astype(jnp.float32)

    def shift(x, s):
        return lax.ppermute(x, "pulse", [(i, (i + s) % n) for i in range(n)])

    order = sorted(range(1, n), key=lambda s: -min(s, n - s))
    got = []
    for channel in range(channels):
        outs = range_compress(n, channel, samples, tw1, rep, tw2, wf, wi)
        blocks = [outs[0]] + [None] * (n - 1)
        for s in order:
            blocks[n - s] = shift(outs[s], s)
        got.append(blocks)

    ratio, sums = None, []
    up = [(i, i + 1) for i in range(n - 1)]
    down = [(i + 1, i) for i in range(n - 1)]
    for channel in range(channels):
        blocks = got[channel]
        if n != RADIX:
            full = jnp.concatenate(blocks, axis=1)
            blocks = [full[:, q * (pulses // RADIX):(q + 1) * (pulses // RADIX)] for q in range(RADIX)]
        power = doppler_power(blocks, table)
        left = lax.ppermute(power[:, :, own - MARGIN:], "pulse", up)
        right = lax.ppermute(power[:, :, :MARGIN], "pulse", down)
        ratio, part_sum = cfar(channel, channels, power, left, right, band, cells, thresh, ratio)
        sums.append(part_sum)
    total = jnp.sum(functools.reduce(jnp.add, sums)) * (1024.0 / (pulses * gates))
    everyone = lax.all_gather(total.reshape(1), ("pulse", "chan", "sub"), tiled=True)
    return (ratio, jnp.sum(everyone).reshape(1))


def solution(mesh):
    in_specs = (
        P(None, ("grp", "chan", "sub"), "pulse", None),
        P(),
        P(("grp", "chan", "sub"), None),
        P(("grp", "chan", "sub"), None),
    )
    out_specs = (P(("grp", "chan", "sub"), None, "pulse"), P("grp"))
    return jax.shard_map(local, mesh=mesh, in_specs=in_specs, out_specs=out_specs, check_vma=False)
```

```python
import functools
import math

import jax
import jax.numpy as jnp
import numpy as np
from jax import lax
from jax.experimental import pallas as pl
from jax.experimental.pallas import tpu as pltpu
from jax.sharding import PartitionSpec as P

GUARD_MAX = 4
TRAIN_MAX = 28
MARGIN = GUARD_MAX + TRAIN_MAX
EPSILON = 1e-06
INPUT_SCALE = 1.0 / 2048.0
LANES = 128
SUB = 8
RADIX = 4


def halves(table):
    hi = np.asarray(table, np.float32).astype(jnp.bfloat16)
    lo = (np.asarray(table, np.float64) - hi.astype(np.float64)).astype(jnp.bfloat16)
    return hi, lo


def lane_table(sign):
    idx = np.arange(LANES)
    ang = 2.0 * np.pi * ((idx[:, None] * idx[None, :]) % LANES) / LANES
    c, s = np.cos(ang), sign * np.sin(ang)
    full = np.block([[c, s], [-s, c]])
    hi, lo = halves(full)
    return np.concatenate([hi, hi, lo], axis=0)


def doppler_table(pulses):
    part = pulses // RADIX
    m = np.arange(part)
    out = []
    for res in range(RADIX):
        ang = 2.0 * np.pi * ((m[None, :] * (RADIX * m[:, None] + res)) % pulses) / pulses
        c, s = np.cos(ang) / math.sqrt(pulses), -np.sin(ang) / math.sqrt(pulses)
        full = np.block([[c, -s], [s, c]])
        hi, lo = halves(full)
        out.append(np.concatenate([hi, hi, lo], axis=1))
    return np.stack(out)


def split(x, axis):
    hi = x.astype(jnp.bfloat16)
    lo = (x - hi.astype(jnp.float32)).astype(jnp.bfloat16)
    return jnp.concatenate([hi, lo, hi], axis=axis)


def fft_list(re, im, sign):
    n = len(re)
    if n == 1:
        return re, im
    er, ei = fft_list(re[0::2], im[0::2], sign)
    odd_r, odd_i = fft_list(re[1::2], im[1::2], sign)
    half = n // 2
    out_r, out_i = [None] * n, [None] * n
    for k in range(half):
        a, b = odd_r[k], odd_i[k]
        if k == 0:
            tr, ti = a, b
        elif 4 * k == n:
            tr, ti = (b, -a) if sign < 0 else (-b, a)
        elif 8 * k == n or 8 * k == 3 * n:
            h = math.sqrt(0.5)
            c = h if 8 * k == n else -h
            tr = c * a - (sign * h) * b
            ti = c * b + (sign * h) * a
        else:
            c = math.cos(2.0 * math.pi * k / n)
            s = sign * math.sin(2.0 * math.pi * k / n)
            tr = c * a - s * b
            ti = s * a + c * b
        out_r[k], out_i[k] = er[k] + tr, ei[k] + ti
        out_r[k + half], out_i[k + half] = er[k] - tr, ei[k] - ti
    return out_r, out_i


def range_kernel(n, rows, x_ref, tw1, rep, tw2, wf, wi, *rest):
    outs = rest[:n]
    cols = x_ref.shape[-1] // LANES
    per = cols // n

    def body(g, carry):
        r0 = pl.multiple_of(g * SUB, SUB)
        re = [x_ref[0, 0, pl.ds(r0, SUB), a * LANES:(a + 1) * LANES].astype(jnp.float32) for a in range(cols)]
        im = [x_ref[1, 0, pl.ds(r0, SUB), a * LANES:(a + 1) * LANES].astype(jnp.float32) for a in range(cols)]
        re, im = fft_list(re, im, -1.0)
        mr, mi = jnp.concatenate(re, axis=0), jnp.concatenate(im, axis=0)
        tr, ti = tw1[0], tw1[1]
        m = jnp.concatenate([mr * tr - mi * ti, mr * ti + mi * tr], axis=1)
        f = jnp.dot(split(m, 1), wf[...], preferred_element_type=jnp.float32)
        fr, fi = f[:, :LANES], f[:, LANES:]
        tr, ti = rep[0], rep[1]
        m = jnp.concatenate([fr * tr - fi * ti, fr * ti + fi * tr], axis=1)
        f = jnp.dot(split(m, 1), wi[...], preferred_element_type=jnp.float32)
        fr, fi = f[:, :LANES], f[:, LANES:]
        tr, ti = tw2[0], tw2[1]
        mr, mi = fr * tr - fi * ti, fr * ti + fi * tr
        re = [mr[a * SUB:(a + 1) * SUB] for a in range(cols)]
        im = [mi[a * SUB:(a + 1) * SUB] for a in range(cols)]
        re, im = fft_list(re, im, 1.0)
        for j in range(n):
            for a in range(per):
                outs[j][0, pl.ds(r0, SUB), a * LANES:(a + 1) * LANES] = re[j * per + a]
                outs[j][1, pl.ds(r0, SUB), a * LANES:(a + 1) * LANES] = im[j * per + a]
        return carry

    lax.fori_loop(0, rows // SUB, body, 0, unroll=2)


def range_compress(n, channel, samples, tw1, rep, tw2, wf, wi):
    _, _, pulses, gates = samples.shape
    rows = min(32, pulses)
    whole = lambda a: pl.BlockSpec(a.shape, lambda i: (0,) * a.ndim)
    return pl.pallas_call(
        functools.partial(range_kernel, n, rows),
        grid=(pulses // rows,),
        in_specs=[pl.BlockSpec((2, 1, rows, gates), lambda i: (0, channel, i, 0))]
        + [whole(a) for a in (tw1, rep, tw2, wf, wi)],
        out_specs=[pl.BlockSpec((2, rows, gates // n), lambda i: (0, i, 0))] * n,
        out_shape=[jax.ShapeDtypeStruct((2, pulses, gates // n), jnp.float32)] * n,
        compiler_params=pltpu.CompilerParams(vmem_limit_bytes=60 << 20),
        cost_estimate=pl.CostEstimate(flops=int(3e9), bytes_accessed=16 << 20, transcendentals=0),
    )(samples, tw1, rep, tw2, wf, wi)


def doppler_kernel(x0, x1, x2, x3, t_ref, p_ref):
    part = x0.shape[1]
    a, b, c, d = ([x[0], x[1]] for x in (x0, x1, x2, x3))
    sr, si = a[0] + c[0], a[1] + c[1]
    dr, di = a[0] - c[0], a[1] - c[1]
    ur, ui = b[0] + d[0], b[1] + d[1]
    vr, vi = b[0] - d[0], b[1] - d[1]
    ys = [(sr + ur, si + ui), (dr + vi, di - vr), (sr - ur, si - ui), (dr - vi, di + vr)]
    for res in range(RADIX):
        y = jnp.concatenate(ys[res], axis=0)
        out = jnp.dot(t_ref[res], split(y, 0), preferred_element_type=jnp.float32)
        re, im = out[:part], out[part:]
        p_ref[res] = re * re + im * im


def doppler_power(blocks, table):
    _, part, gates = blocks[0].shape
    width = min(256, gates)
    return pl.pallas_call(
        doppler_kernel,
        grid=(gates // width,),
        in_specs=[pl.BlockSpec((2, part, width), lambda i: (0, 0, i))] * RADIX
        + [pl.BlockSpec(table.shape, lambda i: (0, 0, 0))],
        out_specs=pl.BlockSpec((RADIX, part, width), lambda i: (0, 0, i)),
        out_shape=jax.ShapeDtypeStruct((RADIX, part, gates), jnp.float32),
        compiler_params=pltpu.CompilerParams(vmem_limit_bytes=40 << 20),
        cost_estimate=pl.CostEstimate(flops=int(3e9), bytes_accessed=8 << 20, transcendentals=0),
    )(*blocks, table)


def cfar_kernel(channel, scale_ref, p_ref, l_ref, r_ref, band_ref, cells_ref, *rest):
    out_ref, sum_ref, turn = rest[-3:]
    _, rows, gates = p_ref.shape
    width = band_ref.shape[-1]
    total = RADIX * rows
    core = p_ref[...].reshape(total, gates)
    zeros = jnp.zeros((total, LANES - MARGIN), jnp.float32)
    padded = jnp.concatenate(
        [zeros, l_ref[...].reshape(total, MARGIN), core, r_ref[...].reshape(total, MARGIN), zeros], axis=1
    )
    hi = padded.astype(jnp.bfloat16)
    lo = (padded - hi.astype(jnp.float32)).astype(jnp.bfloat16)
    band = band_ref[0]
    inv = scale_ref[channel, 1].astype(jnp.float32) / scale_ref[channel, 0].astype(jnp.float32)
    acc = jnp.zeros((SUB, LANES), jnp.float32)
    for g in range(gates // width):
        cut = slice(g * width, (g + 1) * width + 2 * LANES)
        noise = jnp.dot(hi[:, cut], band, preferred_element_type=jnp.float32) + jnp.dot(
            lo[:, cut], band, preferred_element_type=jnp.float32
        )
        here = slice(g * width, (g + 1) * width)
        ratio = core[:, here] * cells_ref[0, :, here] / (noise + EPSILON)
        for c in range(width // LANES):
            lanes = slice(c * LANES, (c + 1) * LANES)
            for res in range(RADIX):
                turn[g, c, pl.ds(res, rows, stride=RADIX), :] = ratio[res * rows:(res + 1) * rows, lanes]
            out_ref[0, :, g * width + c * LANES:g * width + (c + 1) * LANES] = turn[g, c]
        soft = jnp.clip(ratio * inv - 1.0, 0.0, 1.0)
        for c in range(width // LANES):
            acc = acc + jnp.sum(soft[:, c * LANES:(c + 1) * LANES].reshape(total // SUB, SUB, LANES), axis=0)

    @pl.when(pl.program_id(0) == 0)
    def _():
        sum_ref[...] = jnp.zeros_like(sum_ref)

    sum_ref[...] += acc


def cfar(channel, channels, power, left, right, band, cells, thresh, prior):
    _, part, gates = power.shape
    rows = min(32, part)
    width = band.shape[-1]
    specs = [
        pl.BlockSpec(memory_space=pltpu.SMEM),
        pl.BlockSpec((RADIX, rows, gates), lambda i: (0, i, 0)),
        pl.BlockSpec((RADIX, rows, MARGIN), lambda i: (0, i, 0)),
        pl.BlockSpec((RADIX, rows, MARGIN), lambda i: (0, i, 0)),
        pl.BlockSpec((1,) + band.shape[1:], lambda i: (channel, 0, 0)),
        pl.BlockSpec((1,) + cells.shape[1:], lambda i: (channel, 0, 0)),
    ]
    args = [thresh, power, left, right, band, cells]
    aliases = {}
    if prior is not None:
        specs.append(pl.BlockSpec(memory_space=pl.ANY))
        args.append(prior)
        aliases = {6: 0}
    return pl.pallas_call(
        functools.partial(cfar_kernel, channel),
        grid=(part // rows,),
        in_specs=specs,
        out_specs=[
            pl.BlockSpec((1, RADIX * rows, gates), lambda i: (channel, i, 0)),
            pl.BlockSpec((SUB, LANES), lambda i: (0, 0)),
        ],
        out_shape=[
            jax.ShapeDtypeStruct((channels, RADIX * part, gates), jnp.float32),
            jax.ShapeDtypeStruct((SUB, LANES), jnp.float32),
        ],
        input_output_aliases=aliases,
        scratch_shapes=[pltpu.VMEM((gates // width, width // LANES, RADIX * rows, LANES), jnp.float32)],
        compiler_params=pltpu.CompilerParams(vmem_limit_bytes=40 << 20),
        cost_estimate=pl.CostEstimate(flops=int(2e9), bytes_accessed=5 << 20, transcendentals=0),
    )(*args)


def sum_over(x, axis):
    size = lax.axis_size(axis)
    if size & (size - 1):
        return lax.psum(x, axis)
    bit = 1
    while bit < size:
        x = x + lax.ppermute(x, axis, [(i, i ^ bit) for i in range(size)])
        bit *= 2
    return x


def local(samples, replica, window, thresh):
    _, channels, part, gates = samples.shape
    n = lax.axis_size("pulse")
    me = lax.axis_index("pulse")
    cols = gates // LANES
    pulses = part * n
    own = gates // n

    k1 = np.arange(cols)[:, None]
    b = np.arange(LANES)[None, :]
    ang = 2.0 * np.pi * ((k1 * b) % gates) / gates
    tw1 = np.repeat(np.stack([np.cos(ang), -np.sin(ang)]), SUB, axis=1).astype(np.float32)
    turned = (jnp.asarray(k1 * b, jnp.int32) + own * me * jnp.asarray(k1, jnp.int32)) % gates
    ang2 = turned.astype(jnp.float32) * (2.0 * math.pi / gates)
    tw2 = jnp.repeat(jnp.stack([jnp.cos(ang2), jnp.sin(ang2)]), SUB, axis=1)
    rep = jnp.swapaxes(replica.reshape(2, LANES, cols), 1, 2) * (INPUT_SCALE / gates)
    rep = jnp.repeat(rep, SUB, axis=1)
    wf, wi = jnp.asarray(lane_table(-1.0)), jnp.asarray(lane_table(1.0))
    table = jnp.asarray(doppler_table(pulses))

    width = min(256, own)
    guard = window[:, 0][:, None, None]
    reach = guard + window[:, 1][:, None, None]
    dist = jnp.abs(
        jnp.arange(width + 2 * LANES, dtype=jnp.int32)[:, None] - LANES - jnp.arange(width, dtype=jnp.int32)[None, :]
    )[None]
    band = ((dist > guard) & (dist <= reach)).astype(jnp.bfloat16)
    gate = (me * own + jnp.arange(own, dtype=jnp.int32))[None, None, :]
    after = gates - 1 - gate
    cells = (
        jnp.minimum(gate, reach) - jnp.minimum(gate, guard) + jnp.minimum(after, reach) - jnp.minimum(after, guard)
    ).astype(jnp.float32)

    def shift(x, s):
        return lax.ppermute(x, "pulse", [(i, (i + s) % n) for i in range(n)])

    order = sorted(range(1, n), key=lambda s: -min(s, n - s))
    got = []
    for channel in range(channels):
        outs = range_compress(n, channel, samples, tw1, rep, tw2, wf, wi)
        blocks = [outs[0]] + [None] * (n - 1)
        for s in order:
            blocks[n - s] = shift(outs[s], s)
        got.append(blocks)

    ratio, sums = None, []
    up = [(i, i + 1) for i in range(n - 1)]
    down = [(i + 1, i) for i in range(n - 1)]
    for channel in range(channels):
        blocks = got[channel]
        if sums:
            blocks, sums = lax.optimization_barrier((blocks, sums))
        if n != RADIX:
            full = jnp.concatenate(blocks, axis=1)
            blocks = [full[:, q * (pulses // RADIX):(q + 1) * (pulses // RADIX)] for q in range(RADIX)]
        power = doppler_power(blocks, table)
        left = lax.ppermute(power[:, :, own - MARGIN:], "pulse", up)
        right = lax.ppermute(power[:, :, :MARGIN], "pulse", down)
        ratio, part_sum = cfar(channel, channels, power, left, right, band, cells, thresh, ratio)
        sums.append(part_sum)
    total = jnp.sum(functools.reduce(jnp.add, sums)) * (1024.0 / (pulses * gates))
    count = total.reshape(1)
    for axis in ("sub", "chan", "pulse"):
        count = sum_over(count, axis)
    return (ratio, count)


def solution(mesh):
    in_specs = (
        P(None, ("grp", "chan", "sub"), "pulse", None),
        P(),
        P(("grp", "chan", "sub"), None),
        P(("grp", "chan", "sub"), None),
    )
    out_specs = (P(("grp", "chan", "sub"), None, "pulse"), P("grp"))
    return jax.shard_map(local, mesh=mesh, in_specs=in_specs, out_specs=out_specs, check_vma=False)
```
